32 devices in a mesh: gx: 8 (over z, x), gy: 4 (over y, core).
Axes of the slice: x: 2, y: 2, z: 4, core: 2. Of those that a mesh axis runs over, the one named last changes fastest.
Arguments:
- velocity: float32 [3, 64, 256, 256], P(None, 'gx', 'gy'), may hold values from -10 to 10
Outputs:
- coefficient: float32 [256], P('gy')
- viscosity: float32 [64, 256, 256], P('gx', 'gy')
The draws below stay inside these ranges and needn't reach their ends.
All inputs are finite; a program needn't handle non-finite values.
Results may differ from the reference program's by a relative error of at most 0.00002.
Values sent between devices are 32-bit elements; how exact they have to be, the bound alone decides.
No kernel may reach another device: no remote copies, remote signals or barrier semaphores. Data moves between devices by JAX's collectives and lax.ppermute only.
A program may use at most 64 MiB of HBM per device.

```python
import jax
import jax.numpy as jnp
from jax import lax

NZ = 256
NX = 64
NY = 256


def draw_velocity(key, part):
    noise_key = jax.random.fold_in(key, 0)
    stream_pos = jnp.arange(NX, dtype=jnp.float32) / NX
    wall_pos = (jnp.arange(NY, dtype=jnp.float32) + 0.5) / NY
    amplitude = (0.5 + stream_pos)[:, None, None] * (0.5 + wall_pos)[None, :, None]
    fluctuation = jax.random.normal(noise_key, (3, NX, NY, NZ), jnp.float32)
    mean_flow = 6.0 * wall_pos * (1.0 - wall_pos)
    mean_field = jnp.stack([mean_flow, 0.0 * mean_flow, 0.0 * mean_flow])
    velocity_field = amplitude[None] * fluctuation + mean_field[:, None, :, None]
    return jnp.clip(velocity_field, -10.0, 10.0)


def setup_inputs(seed: int = 0) -> dict:
    arg_keys = jax.random.split(jax.random.key(seed), 2)
    velocity = draw_velocity(jax.random.fold_in(arg_keys[1], 71), 0)
    return {"velocity": velocity}


step_stream = 2.0
step_wall = 0.5
step_span = 1.0
clip_high = 0.1
weights = (1.0, 1.0, 1.0, 2.0, 2.0, 2.0)
index_pairs = ((0, 0), (1, 1), (2, 2), (0, 1), (0, 2), (1, 2))

def strain_inner(padded):
    grad_stream = (padded[:, 2:, 1:-1] - padded[:, :-2, 1:-1]) * (0.5 / step_stream)
    grad_wall = (padded[:, 1:-1, 2:] - padded[:, 1:-1, :-2]) * (0.5 / step_wall)
    centre = padded[:, 1:-1, 1:-1]
    grad_span = (jnp.roll(centre, -1, 3) - jnp.roll(centre, 1, 3)) * (0.5 / step_span)
    gradients = (grad_stream, grad_wall, grad_span)
    return jnp.stack([0.5 * (gradients[second][first] + gradients[first][second]) for first, second in index_pairs])

def weight_column():
    return jnp.asarray(weights, jnp.float32).reshape(6, 1, 1, 1)

def magnitude(strain):
    return jnp.sqrt(2.0 * lax.optimization_barrier(jnp.sum(weight_column() * strain * strain, axis=0)))

def test_filter(field):
    smoothed = 0.25 * field[:, :-2] + 0.5 * field[:, 1:-1] + 0.25 * field[:, 2:]
    return 0.25 * jnp.roll(smoothed, 1, 3) + 0.5 * smoothed + 0.25 * jnp.roll(smoothed, -1, 3)

def plane_sums(velocity_pad, stress_pad, filtered_pad):
    strain_hat = strain_inner(filtered_pad)
    magnitude_hat = magnitude(strain_hat)
    row_values = velocity_pad[:, :, 1:-1]
    products = jnp.stack([row_values[first] * row_values[second] for first, second in index_pairs])
    product_hat = test_filter(products)
    centre = filtered_pad[:, 1:-1, 1:-1]
    leonard = product_hat - jnp.stack([centre[first] * centre[second] for first, second in index_pairs])
    trace_third = (leonard[0] + leonard[1] + leonard[2]) / 3.0
    leonard = jnp.concatenate([leonard[:3] - trace_third[None], leonard[3:]])
    model_tensor = 2.0 * (test_filter(stress_pad) - 4.0 * magnitude_hat[None] * strain_hat)
    numerator = lax.optimization_barrier(jnp.sum(weight_column() * leonard * model_tensor, axis=(0, 1, 3)))
    denominator = lax.optimization_barrier(jnp.sum(weight_column() * model_tensor * model_tensor, axis=(0, 1, 3)))
    return (numerator, denominator)

def wrap_stream(field):
    return jnp.concatenate([field[:, -1:], field, field[:, :1]], axis=1)

def pad_walls(field):
    return jnp.pad(field, ((0, 0), (0, 0), (1, 1), (0, 0)))

def reference(velocity):
    velocity_pad = pad_walls(wrap_stream(velocity))
    strain = strain_inner(velocity_pad)
    strength = magnitude(strain)
    stress = strength[None] * strain
    filtered = test_filter(velocity_pad[:, :, 1:-1])
    filtered_pad = pad_walls(wrap_stream(filtered))
    stress_pad = wrap_stream(stress)
    numerator, denominator = plane_sums(velocity_pad, stress_pad, filtered_pad)
    raw_profile = jnp.clip(numerator / denominator, 0.0, clip_high)
    rim_values = jnp.concatenate([raw_profile[:1], raw_profile, raw_profile[-1:]])
    smooth = 0.25 * rim_values[:-2] + 0.5 * raw_profile + 0.25 * rim_values[2:]
    return (smooth, smooth[None, :, None] * strength)
```

```python
import functools

import jax
import jax.numpy as jnp
from jax import lax
from jax.experimental import pallas as pl
from jax.experimental.pallas import tpu as pltpu
from jax.sharding import PartitionSpec as P

clip_high = 0.1
index_pairs = ((0, 0), (1, 1), (2, 2), (0, 1), (0, 2), (1, 2))
scale_x, scale_y, scale_z = 0.25, 1.0, 0.5
TILE = 8


def tile(k):
    return slice(TILE * k, TILE * k + TILE)


def z_pair(value):
    return pltpu.roll(value, 1, 1), pltpu.roll(value, value.shape[1] - 1, 1)


def z_sum(value):
    low, high = z_pair(value)
    return (low + high) + (value + value)


def x_sum(low, value, high):
    return (low + high) + (value + value)


def y_difference(value, row, k, tiles):
    low, high = pltpu.roll(value, 1, 0), pltpu.roll(value, TILE - 1, 0)
    if k < tiles:
        ids = lax.broadcasted_iota(jnp.int32, value.shape, 0)
        before = TILE * k - 1 if k else TILE * tiles + 1
        after = TILE * k + TILE if k < tiles - 1 else TILE * tiles + 5
        low = jnp.where(ids == 0, row(before), low)
        high = jnp.where(ids == TILE - 1, row(after), high)
    return high - low


def strain_of(dx, dy, dz):
    return (
        dx[0] * scale_x,
        dy[1] * scale_y,
        dz[2] * scale_z,
        dy[0] * (0.5 * scale_y) + dx[1] * (0.5 * scale_x),
        dz[0] * (0.5 * scale_z) + dx[2] * (0.5 * scale_x),
        dz[1] * (0.5 * scale_z) + dy[2] * (0.5 * scale_y),
    )


def weighted(a, b):
    diagonal = a[0] * b[0] + a[1] * b[1] + a[2] * b[2]
    off = a[3] * b[3] + a[4] * b[4] + a[5] * b[5]
    return diagonal + (off + off)


def magnitude(strain):
    square = weighted(strain, strain)
    return jnp.sqrt(square + square)


def filter_row(cells, products, smooth, i, tiles, with_products=True):
    for k in range(tiles + 1):
        centre = [cells[c, i, tile(k)] for c in range(3)]
        pairs = [z_pair(value) for value in centre]
        store_filters(centre, pairs, products, smooth, i, k, with_products)


def store_filters(centre, pairs, products, smooth, i, k, with_products=True):
    for c in range(3):
        smooth[c, i, tile(k)] = (pairs[c][0] + pairs[c][1]) + (centre[c] + centre[c])
    if with_products:
        for n, (a, b) in enumerate(index_pairs):
            middle = centre[a] * centre[b]
            products[n, i, tile(k)] = (
                pairs[a][0] * pairs[b][0] + pairs[a][1] * pairs[b][1]
            ) + (middle + middle)


def stress_row(cells, stress, products, smooth, strength, i, s, tiles, filters=True):
    for k in range(tiles + 1):
        centre = [cells[c, i, tile(k)] for c in range(3)]
        pairs = [z_pair(value) for value in centre]
        dx = [cells[c, i + 1, tile(k)] - cells[c, i - 1, tile(k)] for c in range(3)]
        dy = [
            y_difference(centre[c], lambda r, c=c: cells[c, i, r : r + 1], k, tiles)
            for c in range(3)
        ]
        dz = [high - low for low, high in pairs]
        strain = strain_of(dx, dy, dz)
        size = magnitude(strain)
        if strength is not None and k < tiles:
            strength[s, tile(k)] = size
        for n in range(6):
            stress[n, i, tile(k)] = z_sum(size * strain[n])
        if filters:
            store_filters(centre, pairs, products, smooth, i, k)


def smooth_row(smooth, filtered, i, tiles):
    for k in range(tiles + 1):
        for c in range(3):
            filtered[c, i, tile(k)] = (1.0 / 16.0) * x_sum(
                smooth[c, i - 1, tile(k)], smooth[c, i, tile(k)], smooth[c, i + 1, tile(k)]
            )


def model_row(stress, products, filtered, sums, j, tiles):
    for k in range(tiles + 1):
        centre = [filtered[c, j, tile(k)] for c in range(3)]
        dx = [filtered[c, j + 1, tile(k)] - filtered[c, j - 1, tile(k)] for c in range(3)]
        dy = [
            y_difference(centre[c], lambda r, c=c: filtered[c, j, r : r + 1], k, tiles)
            for c in range(3)
        ]
        dz = []
        for c in range(3):
            low, high = z_pair(centre[c])
            dz.append(high - low)
        strain = strain_of(dx, dy, dz)
        size = 64.0 * magnitude(strain)
        model = [
            x_sum(stress[n, j - 1, tile(k)], stress[n, j, tile(k)], stress[n, j + 1, tile(k)])
            - size * strain[n]
            for n in range(6)
        ]
        leonard = [
            (1.0 / 16.0)
            * x_sum(products[n, j - 1, tile(k)], products[n, j, tile(k)], products[n, j + 1, tile(k)])
            - centre[a] * centre[b]
            for n, (a, b) in enumerate(index_pairs)
        ]
        third = (leonard[0] + leonard[1] + leonard[2]) * (1.0 / 3.0)
        leonard = [value - third for value in leonard[:3]] + leonard[3:]
        sums[0, tile(k)] += weighted(leonard, model)
        sums[1, tile(k)] += weighted(model, model)


def loop(start, stop, body):
    def step(i, carry):
        body(i)
        return carry

    lax.fori_loop(start, stop, step, 0)


def edge_tiles(cells, low, high, i, rows):
    first, last = cells[:, i, :1], cells[:, i, rows - 1 : rows]
    zero = jnp.zeros_like(first)
    cells[:, i, rows:] = jnp.concatenate([low, first, zero, last, high, zero], axis=1)


def copies(pairs, sems, base=0):
    return [pltpu.make_async_copy(a, b, sems.at[base + n]) for n, (a, b) in enumerate(pairs)]


def start(work):
    for copy in work:
        copy.start()


def wait(work):
    for copy in work:
        copy.wait()


def kept_rows(own):
    return (
        ((3, 2), (own - 1, 2)),
        ((2, 3), (own - 1, 3)),
        ((2, 2), (own, 2)),
        ((3, 2), (own - 1, 2)),
    )


def kept_pairs(fields, keeps, own):
    out = []
    for field, keep, spans in zip(fields, keeps, kept_rows(own)):
        offset = 0
        for at, count in spans:
            out.append((field.at[:, at : at + count], keep.at[:, offset : offset + count]))
            offset += count
    return out


def inner_kernel(
    v, low, high, sums, strength, stress_keep, products_keep, smooth_keep, filtered_keep,
    stress, products, smooth, filtered, cells, sems,
):
    own, rows = v.shape[1], v.shape[2]
    tiles = rows // TILE
    load = copies([(v, cells.at[:, 2 : own + 2, :rows])], sems)
    start(load)
    sums[...] = jnp.zeros_like(sums)
    wait(load)
    for i in range(own):
        edge_tiles(cells, low[:, i], high[:, i], i + 2, rows)
    loop(0, 2, lambda s: filter_row(cells, products, smooth, 2 + s * (own - 1), tiles))
    loop(
        3,
        own + 1,
        lambda i: stress_row(cells, stress, products, smooth, strength, i, i - 3, tiles),
    )
    loop(3, own + 1, lambda i: smooth_row(smooth, filtered, i, tiles))
    keeps = (stress_keep, products_keep, smooth_keep, filtered_keep)
    save = copies(kept_pairs((stress, products, smooth, filtered), keeps, own), sems, 1)
    start(save[:6])
    loop(4, own, lambda j: model_row(stress, products, filtered, sums, j, tiles))
    start(save[6:])
    wait(save)


def outer_kernel(
    v, left, right, low, high, left_edge, right_edge,
    stress_keep, products_keep, smooth_keep, filtered_keep, sums_in,
    totals, strength,
    stress, products, smooth, filtered, sums, cells, sems,
):
    own, rows = v.shape[1], v.shape[2]
    tiles = rows // TILE
    ends = [
        (left, cells.at[:, 0:2, :rows]),
        (v.at[:, 0:2], cells.at[:, 2:4, :rows]),
        (v.at[:, own - 2 : own], cells.at[:, own : own + 2, :rows]),
        (right, cells.at[:, own + 2 : own + 4, :rows]),
    ]
    load = copies(ends, sems)
    start(load)
    keeps = (stress_keep, products_keep, smooth_keep, filtered_keep)
    kept = kept_pairs((stress, products, smooth, filtered), keeps, own)
    more = copies([(b, a) for a, b in kept], sems, 4)
    start(more)
    sums[...] = sums_in[...]
    wait(load)
    for i in range(2):
        edge_tiles(cells, left_edge[:, i, :2], left_edge[:, i, 2:], i, rows)
        edge_tiles(cells, low[:, i], high[:, i], i + 2, rows)
        edge_tiles(cells, low[:, own - 2 + i], high[:, own - 2 + i], own + i, rows)
        edge_tiles(cells, right_edge[:, i, :2], right_edge[:, i, 2:], own + 2 + i, rows)

    def side(s):
        filter_row(cells, products, smooth, s * (own + 3), tiles, with_products=False)
        stress_row(cells, stress, products, smooth, None, 1 + s * (own + 1), s, tiles)

    loop(0, 2, side)
    loop(
        0,
        2,
        lambda s: stress_row(
            cells, stress, products, smooth, strength, 2 + s * (own - 1), s, tiles, False
        ),
    )
    wait(more)
    loop(0, 4, lambda t: smooth_row(smooth, filtered, 1 + t + (t // 2) * (own - 2), tiles))
    loop(
        0,
        4,
        lambda t: model_row(
            stress, products, filtered, sums, 2 + t + (t // 2) * (own - 4), tiles
        ),
    )
    for n in range(2):
        value = sums[n]
        folded = value[:, : value.shape[1] // 2] + value[:, value.shape[1] // 2 :]
        totals[n : n + 1] = jnp.sum(folded.T, axis=0, keepdims=True)


def shift(count, step, closed):
    pairs = [(i, i + step) for i in range(count)]
    if closed:
        return [(i, j % count) for i, j in pairs]
    return [(i, j) for i, j in pairs if 0 <= j < count]


def vmem(n):
    return [pl.BlockSpec(memory_space=pltpu.VMEM)] * n


def anywhere(n):
    return [pl.BlockSpec(memory_space=pl.ANY)] * n


def sum_over(value, axis):
    count = lax.axis_size(axis)
    if count & (count - 1):
        return lax.psum(value, axis)
    step = 1
    while step < count:
        value = value + lax.ppermute(value, axis, [(i, i ^ step) for i in range(count)])
        step *= 2
    return value


def local(v):
    _, own, rows, span = v.shape
    wall_count = lax.axis_size("gy")
    stream_count = lax.axis_size("gx")
    wall_index = lax.axis_index("gy")
    float_array = functools.partial(jax.ShapeDtypeStruct, dtype=jnp.float32)

    to_next = shift(stream_count, 1, True)
    to_last = shift(stream_count, -1, True)
    left = lax.ppermute(v[:, own - 2 :], "gx", to_next)
    right = lax.ppermute(v[:, :2], "gx", to_last)
    low = lax.ppermute(v[:, :, rows - 2 :], "gy", shift(wall_count, 1, False))
    high = lax.ppermute(v[:, :, :2], "gy", shift(wall_count, -1, False))
    edges = jnp.concatenate([low, high], axis=2)
    left_edge = lax.ppermute(edges[:, own - 2 :], "gx", to_next)
    right_edge = lax.ppermute(edges[:, :2], "gx", to_last)

    tall = rows + TILE
    wide = own + 4
    kept = tuple(
        float_array((fields, sum(count for _, count in spans), tall, span))
        for fields, spans in zip((6, 6, 3, 3), kept_rows(own))
    )
    fields = [pltpu.VMEM((n, wide, tall, span), jnp.float32) for n in (6, 6, 3, 3)]
    cells = pltpu.VMEM((3, wide, tall, span), jnp.float32)
    params = pltpu.CompilerParams(vmem_limit_bytes=30 * 1024 * 1024)
    inner = pl.pallas_call(
        inner_kernel,
        out_shape=(float_array((2, tall, span)), float_array((own - 2, rows, span))) + kept,
        in_specs=anywhere(1) + vmem(2),
        out_specs=tuple(vmem(2) + anywhere(4)),
        scratch_shapes=fields + [cells, pltpu.SemaphoreType.DMA((9,))],
        compiler_params=params,
        cost_estimate=pl.CostEstimate(flops=60_000_000, transcendentals=0, bytes_accessed=6_000_000),
        name="inner",
    )(v, low, high)
    sums, strength_inner = inner[:2]
    totals, strength_outer = pl.pallas_call(
        outer_kernel,
        out_shape=(float_array((2, tall)), float_array((2, rows, span))),
        in_specs=anywhere(3) + vmem(4) + anywhere(4) + vmem(1),
        out_specs=tuple(vmem(2)),
        scratch_shapes=fields
        + [pltpu.VMEM((2, tall, span), jnp.float32), cells, pltpu.SemaphoreType.DMA((12,))],
        compiler_params=params,
        cost_estimate=pl.CostEstimate(flops=40_000_000, transcendentals=0, bytes_accessed=6_000_000),
        name="outer",
    )(v, left, right, low, high, left_edge, right_edge, *inner[2:], sums)

    totals = sum_over(totals, "gx")
    raw = jnp.clip(8.0 * totals[0] / totals[1], 0.0, clip_high)
    inside = raw[:rows]
    bottom = jnp.where(wall_index == 0, raw[:1], raw[rows + 1 : rows + 2])
    top = jnp.where(wall_index == wall_count - 1, raw[rows - 1 : rows], raw[rows + 5 : rows + 6])
    around = jnp.concatenate([bottom, inside, top])
    coefficient = 0.25 * around[:-2] + 0.5 * inside + 0.25 * around[2:]
    strength = jnp.concatenate([strength_outer[:1], strength_inner, strength_outer[1:]])
    return coefficient, coefficient[None, :, None] * strength


def solution(mesh):
    in_specs = (P(None, "gx", "gy", None),)
    out_specs = (P("gy"), P("gx", "gy", None))
    return jax.shard_map(local, mesh=mesh, in_specs=in_specs, out_specs=out_specs, check_vma=False)
```

```python
import functools

import jax
import jax.numpy as jnp
from jax import lax
from jax.experimental import pallas as pl
from jax.experimental.pallas import tpu as pltpu
from jax.sharding import PartitionSpec as P


clip_high = 0.1
index_pairs = ((0, 0), (1, 1), (2, 2), (0, 1), (0, 2), (1, 2))
scale_x, scale_y, scale_z = 0.25, 1.0, 0.5
TILE = 8


def tile(k):
    return slice(TILE * k, TILE * k + TILE)


def z_pair(value):
    return pltpu.roll(value, 1, 1), pltpu.roll(value, value.shape[1] - 1, 1)


def z_sum(value):
    low, high = z_pair(value)
    return (low + high) + (value + value)


def x_sum(low, value, high):
    return (low + high) + (value + value)


def y_difference(value, row, k, tiles):
    low, high = pltpu.roll(value, 1, 0), pltpu.roll(value, TILE - 1, 0)
    if k < tiles:
        ids = lax.broadcasted_iota(jnp.int32, value.shape, 0)
        before = TILE * k - 1 if k else TILE * tiles + 1
        after = TILE * k + TILE if k < tiles - 1 else TILE * tiles + 5
        low = jnp.where(ids == 0, row(before), low)
        high = jnp.where(ids == TILE - 1, row(after), high)
    return high - low


def strain_of(dx, dy, dz):
    return (
        dx[0] * scale_x,
        dy[1] * scale_y,
        dz[2] * scale_z,
        dy[0] * (0.5 * scale_y) + dx[1] * (0.5 * scale_x),
        dz[0] * (0.5 * scale_z) + dx[2] * (0.5 * scale_x),
        dz[1] * (0.5 * scale_z) + dy[2] * (0.5 * scale_y),
    )


def weighted(a, b):
    diagonal = a[0] * b[0] + a[1] * b[1] + a[2] * b[2]
    off = a[3] * b[3] + a[4] * b[4] + a[5] * b[5]
    return diagonal + (off + off)


def magnitude(strain):
    square = weighted(strain, strain)
    return jnp.sqrt(square + square)


def filter_row(cells, products, smooth, i, tiles, with_products=True):
    for k in range(tiles + 1):
        centre = [cells[c, i, tile(k)] for c in range(3)]
        pairs = [z_pair(value) for value in centre]
        store_filters(centre, pairs, products, smooth, i, k, with_products)


def store_filters(centre, pairs, products, smooth, i, k, with_products=True):
    for c in range(3):
        smooth[c, i, tile(k)] = (pairs[c][0] + pairs[c][1]) + (centre[c] + centre[c])
    if with_products:
        for n, (a, b) in enumerate(index_pairs):
            middle = centre[a] * centre[b]
            products[n, i, tile(k)] = (
                pairs[a][0] * pairs[b][0] + pairs[a][1] * pairs[b][1]
            ) + (middle + middle)


def stress_row(cells, stress, products, smooth, strength, i, s, tiles, filters=True):
    for k in range(tiles + 1):
        centre = [cells[c, i, tile(k)] for c in range(3)]
        pairs = [z_pair(value) for value in centre]
        dx = [cells[c, i + 1, tile(k)] - cells[c, i - 1, tile(k)] for c in range(3)]
        dy = [
            y_difference(centre[c], lambda r, c=c: cells[c, i, r : r + 1], k, tiles)
            for c in range(3)
        ]
        dz = [high - low for low, high in pairs]
        strain = strain_of(dx, dy, dz)
        size = magnitude(strain)
        if strength is not None and k < tiles:
            strength[s, tile(k)] = size
        for n in range(6):
            stress[n, i, tile(k)] = z_sum(size * strain[n])
        if filters:
            store_filters(centre, pairs, products, smooth, i, k)


def smooth_row(smooth, filtered, i, tiles):
    for k in range(tiles + 1):
        for c in range(3):
            filtered[c, i, tile(k)] = (1.0 / 16.0) * x_sum(
                smooth[c, i - 1, tile(k)], smooth[c, i, tile(k)], smooth[c, i + 1, tile(k)]
            )


def model_row(stress, products, filtered, sums, j, tiles):
    for k in range(tiles + 1):
        centre = [filtered[c, j, tile(k)] for c in range(3)]
        dx = [filtered[c, j + 1, tile(k)] - filtered[c, j - 1, tile(k)] for c in range(3)]
        dy = [
            y_difference(centre[c], lambda r, c=c: filtered[c, j, r : r + 1], k, tiles)
            for c in range(3)
        ]
        dz = []
        for c in range(3):
            low, high = z_pair(centre[c])
            dz.append(high - low)
        strain = strain_of(dx, dy, dz)
        size = 64.0 * magnitude(strain)
        model = [
            x_sum(stress[n, j - 1, tile(k)], stress[n, j, tile(k)], stress[n, j + 1, tile(k)])
            - size * strain[n]
            for n in range(6)
        ]
        leonard = [
            (1.0 / 16.0)
            * x_sum(products[n, j - 1, tile(k)], products[n, j, tile(k)], products[n, j + 1, tile(k)])
            - centre[a] * centre[b]
            for n, (a, b) in enumerate(index_pairs)
        ]
        third = (leonard[0] + leonard[1] + leonard[2]) * (1.0 / 3.0)
        leonard = [value - third for value in leonard[:3]] + leonard[3:]
        sums[0, tile(k)] += weighted(leonard, model)
        sums[1, tile(k)] += weighted(model, model)


def loop(start, stop, body):
    def step(i, carry):
        body(i)
        return carry

    lax.fori_loop(start, stop, step, 0)


def edge_tiles(cells, low, high, i, rows):
    first, last = cells[:, i, :1], cells[:, i, rows - 1 : rows]
    zero = jnp.zeros_like(first)
    cells[:, i, rows:] = jnp.concatenate([low, first, zero, last, high, zero], axis=1)


def copies(pairs, sems, base=0):
    return [pltpu.make_async_copy(a, b, sems.at[base + n]) for n, (a, b) in enumerate(pairs)]


def start(work):
    for copy in work:
        copy.start()


def wait(work):
    for copy in work:
        copy.wait()


def kept_rows(own):
    return (
        ((3, 2), (own - 1, 2)),
        ((2, 3), (own - 1, 3)),
        ((2, 2), (own, 2)),
        ((3, 2), (own - 1, 2)),
    )


def kept_pairs(fields, keeps, own):
    out = []
    for field, keep, spans in zip(fields, keeps, kept_rows(own)):
        offset = 0
        for at, count in spans:
            out.append((field.at[:, at : at + count], keep.at[:, offset : offset + count]))
            offset += count
    return out


def inner_kernel(
    v, low, high, sums, strength, stress_keep, products_keep, smooth_keep, filtered_keep,
    stress, products, smooth, filtered, cells, sems,
):
    own, rows = v.shape[1], v.shape[2]
    tiles = rows // TILE
    load = copies([(v, cells.at[:, 2 : own + 2, :rows])], sems)
    start(load)
    sums[...] = jnp.zeros_like(sums)
    wait(load)
    for i in range(own):
        edge_tiles(cells, low[:, i], high[:, i], i + 2, rows)
    loop(0, 2, lambda s: filter_row(cells, products, smooth, 2 + s * (own - 1), tiles))
    loop(
        3,
        own + 1,
        lambda i: stress_row(cells, stress, products, smooth, strength, i, i - 3, tiles),
    )
    loop(3, own + 1, lambda i: smooth_row(smooth, filtered, i, tiles))
    keeps = (stress_keep, products_keep, smooth_keep, filtered_keep)
    save = copies(kept_pairs((stress, products, smooth, filtered), keeps, own), sems, 1)
    start(save[:6])
    loop(4, own, lambda j: model_row(stress, products, filtered, sums, j, tiles))
    start(save[6:])
    wait(save)


def outer_kernel(
    v, left, right, low, high, left_edge, right_edge,
    stress_keep, products_keep, smooth_keep, filtered_keep, sums_in,
    totals, strength,
    stress, products, smooth, filtered, sums, cells, sems,
):
    own, rows = v.shape[1], v.shape[2]
    tiles = rows // TILE
    ends = [
        (left, cells.at[:, 0:2, :rows]),
        (v.at[:, 0:2], cells.at[:, 2:4, :rows]),
        (v.at[:, own - 2 : own], cells.at[:, own : own + 2, :rows]),
        (right, cells.at[:, own + 2 : own + 4, :rows]),
    ]
    load = copies(ends, sems)
    start(load)
    keeps = (stress_keep, products_keep, smooth_keep, filtered_keep)
    kept = kept_pairs((stress, products, smooth, filtered), keeps, own)
    more = copies([(b, a) for a, b in kept], sems, 4)
    start(more)
    sums[...] = sums_in[...]
    wait(load)
    for i in range(2):
        edge_tiles(cells, left_edge[:, i, :2], left_edge[:, i, 2:], i, rows)
        edge_tiles(cells, low[:, i], high[:, i], i + 2, rows)
        edge_tiles(cells, low[:, own - 2 + i], high[:, own - 2 + i], own + i, rows)
        edge_tiles(cells, right_edge[:, i, :2], right_edge[:, i, 2:], own + 2 + i, rows)

    def side(s):
        filter_row(cells, products, smooth, s * (own + 3), tiles, with_products=False)
        stress_row(cells, stress, products, smooth, None, 1 + s * (own + 1), s, tiles)

    loop(0, 2, side)
    loop(
        0,
        2,
        lambda s: stress_row(
            cells, stress, products, smooth, strength, 2 + s * (own - 1), s, tiles, False
        ),
    )
    wait(more)
    loop(0, 4, lambda t: smooth_row(smooth, filtered, 1 + t + (t // 2) * (own - 2), tiles))
    loop(
        0,
        4,
        lambda t: model_row(
            stress, products, filtered, sums, 2 + t + (t // 2) * (own - 4), tiles
        ),
    )
    for n in range(2):
        value = sums[n]
        folded = value[:, : value.shape[1] // 2] + value[:, value.shape[1] // 2 :]
        totals[n : n + 1] = jnp.sum(folded.T, axis=0, keepdims=True)


def final_kernel(totals, strength_inner, strength_outer, coefficient, viscosity):
    own, rows = viscosity.shape[0], viscosity.shape[1]
    tall = totals.shape[1]
    wall_index, wall_count = lax.axis_index("gy"), lax.axis_size("gy")
    raw = jnp.clip(8.0 * totals[0:1] / totals[1:2], 0.0, clip_high)
    plane = lax.broadcasted_iota(jnp.int32, (rows, tall), 0)
    entry = lax.broadcasted_iota(jnp.int32, (rows, tall), 1)
    below = jnp.where(plane == 0, jnp.where(wall_index == 0, 0, rows + 1), plane - 1)
    last = plane == rows - 1
    above = jnp.where(last, jnp.where(wall_index == wall_count - 1, rows - 1, rows + 5), plane + 1)
    spread = jnp.broadcast_to(raw, (rows, tall))
    parts = [
        jnp.where(entry == pick, spread * weight, 0.0)
        for pick, weight in ((below, 0.25), (plane, 0.5), (above, 0.25))
    ]
    column = jnp.sum((parts[0] + parts[2]) + parts[1], axis=1, keepdims=True)
    square = jnp.where(plane[:, :rows] == entry[:, :rows], column, 0.0)
    coefficient[...] = jnp.sum(square, axis=0, keepdims=True)
    for i in range(own):
        source = strength_outer[i // (own - 1)] if i in (0, own - 1) else strength_inner[i - 1]
        viscosity[i] = column * source


def shift(count, step, closed):
    pairs = [(i, i + step) for i in range(count)]
    if closed:
        return [(i, j % count) for i, j in pairs]
    return [(i, j) for i, j in pairs if 0 <= j < count]


def vmem(n):
    return [pl.BlockSpec(memory_space=pltpu.VMEM)] * n


def anywhere(n):
    return [pl.BlockSpec(memory_space=pl.ANY)] * n


def sum_over(value, axis):
    count = lax.axis_size(axis)
    if count & (count - 1):
        return lax.psum(value, axis)
    step = 1
    while step < count:
        value = value + lax.ppermute(value, axis, [(i, i ^ step) for i in range(count)])
        step *= 2
    return value


def local(v):
    _, own, rows, span = v.shape
    wall_count = lax.axis_size("gy")
    stream_count = lax.axis_size("gx")
    float_array = functools.partial(jax.ShapeDtypeStruct, dtype=jnp.float32)

    to_next = shift(stream_count, 1, True)
    to_last = shift(stream_count, -1, True)
    low = lax.ppermute(v[:, :, rows - 2 :], "gy", shift(wall_count, 1, False))
    high = lax.ppermute(v[:, :, :2], "gy", shift(wall_count, -1, False))
    left = lax.ppermute(v[:, own - 2 :], "gx", to_next)
    right = lax.ppermute(v[:, :2], "gx", to_last)
    edges = jnp.concatenate([low, high], axis=2)
    left_edge = lax.ppermute(edges[:, own - 2 :], "gx", to_next)
    right_edge = lax.ppermute(edges[:, :2], "gx", to_last)

    tall = rows + TILE
    wide = own + 4
    kept = tuple(
        float_array((fields, sum(count for _, count in spans), tall, span))
        for fields, spans in zip((6, 6, 3, 3), kept_rows(own))
    )
    fields = [pltpu.VMEM((n, wide, tall, span), jnp.float32) for n in (6, 6, 3, 3)]
    cells = pltpu.VMEM((3, wide, tall, span), jnp.float32)
    params = pltpu.CompilerParams(vmem_limit_bytes=30 * 1024 * 1024)
    inner = pl.pallas_call(
        inner_kernel,
        out_shape=(float_array((2, tall, span)), float_array((own - 2, rows, span))) + kept,
        in_specs=anywhere(1) + vmem(2),
        out_specs=tuple(vmem(2) + anywhere(4)),
        scratch_shapes=fields + [cells, pltpu.SemaphoreType.DMA((9,))],
        compiler_params=params,
        cost_estimate=pl.CostEstimate(flops=60_000_000, transcendentals=0, bytes_accessed=6_000_000),
        name="inner",
    )(v, low, high)
    sums, strength_inner = inner[:2]
    totals, strength_outer = pl.pallas_call(
        outer_kernel,
        out_shape=(float_array((2, tall)), float_array((2, rows, span))),
        in_specs=anywhere(3) + vmem(4) + anywhere(4) + vmem(1),
        out_specs=tuple(vmem(2)),
        scratch_shapes=fields
        + [pltpu.VMEM((2, tall, span), jnp.float32), cells, pltpu.SemaphoreType.DMA((12,))],
        compiler_params=params,
        cost_estimate=pl.CostEstimate(flops=40_000_000, transcendentals=0, bytes_accessed=6_000_000),
        name="outer",
    )(v, left, right, low, high, left_edge, right_edge, *inner[2:], sums)

    totals = sum_over(totals, "gx")
    coefficient, viscosity = pl.pallas_call(
        final_kernel,
        out_shape=(float_array((1, rows)), float_array((own, rows, span))),
        in_specs=vmem(3),
        out_specs=tuple(vmem(2)),
        compiler_params=pltpu.CompilerParams(vmem_limit_bytes=8 * 1024 * 1024),
        name="final",
    )(totals, strength_inner, strength_outer)
    return coefficient[0], viscosity


def solution(mesh):
    in_specs = (P(None, "gx", "gy", None),)
    out_specs = (P("gy"), P("gx", "gy", None))
    return jax.shard_map(local, mesh=mesh, in_specs=in_specs, out_specs=out_specs, check_vma=False)
```

```python
import functools

import jax
import jax.numpy as jnp
from jax import lax
from jax.experimental import pallas as pl
from jax.experimental.pallas import tpu as pltpu
from jax.sharding import PartitionSpec as P


clip_high = 0.1
index_pairs = ((0, 0), (1, 1), (2, 2), (0, 1), (0, 2), (1, 2))
scale_x, scale_y, scale_z = 0.25, 1.0, 0.5
TILE = 8


def tile(k):
    return slice(TILE * k, TILE * k + TILE)


def z_pair(value):
    return pltpu.roll(value, 1, 1), pltpu.roll(value, value.shape[1] - 1, 1)


def z_sum(value):
    low, high = z_pair(value)
    return (low + high) + (value + value)


def x_sum(low, value, high):
    return (low + high) + (value + value)


def y_difference(value, row, k, tiles):
    low, high = pltpu.roll(value, 1, 0), pltpu.roll(value, TILE - 1, 0)
    if k < tiles:
        ids = lax.broadcasted_iota(jnp.int32, value.shape, 0)
        before = TILE * k - 1 if k else TILE * tiles + 1
        after = TILE * k + TILE if k < tiles - 1 else TILE * tiles + 5
        low = jnp.where(ids == 0, row(before), low)
        high = jnp.where(ids == TILE - 1, row(after), high)
    return high - low


def strain_of(dx, dy, dz):
    return (
        dx[0] * scale_x,
        dy[1] * scale_y,
        dz[2] * scale_z,
        dy[0] * (0.5 * scale_y) + dx[1] * (0.5 * scale_x),
        dz[0] * (0.5 * scale_z) + dx[2] * (0.5 * scale_x),
        dz[1] * (0.5 * scale_z) + dy[2] * (0.5 * scale_y),
    )


def weighted(a, b):
    diagonal = a[0] * b[0] + a[1] * b[1] + a[2] * b[2]
    off = a[3] * b[3] + a[4] * b[4] + a[5] * b[5]
    return diagonal + (off + off)


def magnitude(strain):
    square = weighted(strain, strain)
    return jnp.sqrt(square + square)


def filter_row(cells, products, smooth, i, tiles, with_products=True):
    for k in range(tiles + 1):
        centre = [cells[c, i, tile(k)] for c in range(3)]
        pairs = [z_pair(value) for value in centre]
        store_filters(centre, pairs, products, smooth, i, k, with_products)


def store_filters(centre, pairs, products, smooth, i, k, with_products=True):
    for c in range(3):
        smooth[c, i, tile(k)] = (pairs[c][0] + pairs[c][1]) + (centre[c] + centre[c])
    if with_products:
        for n, (a, b) in enumerate(index_pairs):
            middle = centre[a] * centre[b]
            products[n, i, tile(k)] = (
                pairs[a][0] * pairs[b][0] + pairs[a][1] * pairs[b][1]
            ) + (middle + middle)


def stress_row(cells, stress, products, smooth, strength, i, s, tiles, filters=True):
    for k in range(tiles + 1):
        centre = [cells[c, i, tile(k)] for c in range(3)]
        pairs = [z_pair(value) for value in centre]
        dx = [cells[c, i + 1, tile(k)] - cells[c, i - 1, tile(k)] for c in range(3)]
        dy = [
            y_difference(centre[c], lambda r, c=c: cells[c, i, r : r + 1], k, tiles)
            for c in range(3)
        ]
        dz = [high - low for low, high in pairs]
        strain = strain_of(dx, dy, dz)
        size = magnitude(strain)
        if strength is not None and k < tiles:
            strength[s, tile(k)] = size
        for n in range(6):
            stress[n, i, tile(k)] = z_sum(size * strain[n])
        if filters:
            store_filters(centre, pairs, products, smooth, i, k)


def smooth_row(smooth, filtered, i, tiles):
    for k in range(tiles + 1):
        for c in range(3):
            filtered[c, i, tile(k)] = (1.0 / 16.0) * x_sum(
                smooth[c, i - 1, tile(k)], smooth[c, i, tile(k)], smooth[c, i + 1, tile(k)]
            )


def model_row(stress, products, filtered, sums, j, tiles):
    for k in range(tiles + 1):
        centre = [filtered[c, j, tile(k)] for c in range(3)]
        dx = [filtered[c, j + 1, tile(k)] - filtered[c, j - 1, tile(k)] for c in range(3)]
        dy = [
            y_difference(centre[c], lambda r, c=c: filtered[c, j, r : r + 1], k, tiles)
            for c in range(3)
        ]
        dz = []
        for c in range(3):
            low, high = z_pair(centre[c])
            dz.append(high - low)
        strain = strain_of(dx, dy, dz)
        size = 64.0 * magnitude(strain)
        model = [
            x_sum(stress[n, j - 1, tile(k)], stress[n, j, tile(k)], stress[n, j + 1, tile(k)])
            - size * strain[n]
            for n in range(6)
        ]
        leonard = [
            (1.0 / 16.0)
            * x_sum(products[n, j - 1, tile(k)], products[n, j, tile(k)], products[n, j + 1, tile(k)])
            - centre[a] * centre[b]
            for n, (a, b) in enumerate(index_pairs)
        ]
        third = (leonard[0] + leonard[1] + leonard[2]) * (1.0 / 3.0)
        leonard = [value - third for value in leonard[:3]] + leonard[3:]
        sums[0, tile(k)] += weighted(leonard, model)
        sums[1, tile(k)] += weighted(model, model)


def loop(start, stop, body):
    def step(i, carry):
        body(i)
        return carry

    lax.fori_loop(start, stop, step, 0)


def edge_tiles(cells, low, high, i, rows):
    first, last = cells[:, i, :1], cells[:, i, rows - 1 : rows]
    zero = jnp.zeros_like(first)
    cells[:, i, rows:] = jnp.concatenate([low, first, zero, last, high, zero], axis=1)


def copies(pairs, sems, base=0):
    return [pltpu.make_async_copy(a, b, sems.at[base + n]) for n, (a, b) in enumerate(pairs)]


def start(work):
    for copy in work:
        copy.start()


def wait(work):
    for copy in work:
        copy.wait()


def kept_rows(own):
    return (
        ((3, 2), (own - 1, 2)),
        ((2, 3), (own - 1, 3)),
        ((2, 2), (own, 2)),
        ((3, 2), (own - 1, 2)),
    )


def kept_pairs(fields, keeps, own):
    out = []
    for field, keep, spans in zip(fields, keeps, kept_rows(own)):
        offset = 0
        for at, count in spans:
            out.append((field.at[:, at : at + count], keep.at[:, offset : offset + count]))
            offset += count
    return out


def inner_kernel(
    v, low, high, sums, strength, stress_keep, products_keep, smooth_keep, filtered_keep,
    stress, products, smooth, filtered, cells, sems,
):
    own, rows = v.shape[1], v.shape[2]
    tiles = rows // TILE
    load = copies([(v, cells.at[:, 2 : own + 2, :rows])], sems)
    start(load)
    sums[...] = jnp.zeros_like(sums)
    wait(load)
    for i in range(own):
        edge_tiles(cells, low[:, i], high[:, i], i + 2, rows)
    loop(0, 2, lambda s: filter_row(cells, products, smooth, 2 + s * (own - 1), tiles))
    loop(
        3,
        own + 1,
        lambda i: stress_row(cells, stress, products, smooth, strength, i, i - 3, tiles),
    )
    loop(3, own + 1, lambda i: smooth_row(smooth, filtered, i, tiles))
    keeps = (stress_keep, products_keep, smooth_keep, filtered_keep)
    save = copies(kept_pairs((stress, products, smooth, filtered), keeps, own), sems, 1)
    start(save[:6])
    loop(4, own, lambda j: model_row(stress, products, filtered, sums, j, tiles))
    start(save[6:])
    wait(save)


def outer_kernel(
    v, left, right, low, high, left_edge, right_edge,
    stress_keep, products_keep, smooth_keep, filtered_keep, sums_in,
    totals, strength,
    stress, products, smooth, filtered, sums, cells, sems,
):
    own, rows = v.shape[1], v.shape[2]
    tiles = rows // TILE
    ends = [
        (left, cells.at[:, 0:2, :rows]),
        (v.at[:, 0:2], cells.at[:, 2:4, :rows]),
        (v.at[:, own - 2 : own], cells.at[:, own : own + 2, :rows]),
        (right, cells.at[:, own + 2 : own + 4, :rows]),
    ]
    load = copies(ends, sems)
    start(load)
    keeps = (stress_keep, products_keep, smooth_keep, filtered_keep)
    kept = kept_pairs((stress, products, smooth, filtered), keeps, own)
    more = copies([(b, a) for a, b in kept], sems, 4)
    start(more)
    sums[...] = sums_in[...]
    wait(load)
    for i in range(2):
        edge_tiles(cells, left_edge[:, i, :2], left_edge[:, i, 2:], i, rows)
        edge_tiles(cells, low[:, i], high[:, i], i + 2, rows)
        edge_tiles(cells, low[:, own - 2 + i], high[:, own - 2 + i], own + i, rows)
        edge_tiles(cells, right_edge[:, i, :2], right_edge[:, i, 2:], own + 2 + i, rows)

    def side(s):
        filter_row(cells, products, smooth, s * (own + 3), tiles, with_products=False)
        stress_row(cells, stress, products, smooth, None, 1 + s * (own + 1), s, tiles)

    loop(0, 2, side)
    loop(
        0,
        2,
        lambda s: stress_row(
            cells, stress, products, smooth, strength, 2 + s * (own - 1), s, tiles, False
        ),
    )
    wait(more)
    loop(0, 4, lambda t: smooth_row(smooth, filtered, 1 + t + (t // 2) * (own - 2), tiles))
    loop(
        0,
        4,
        lambda t: model_row(
            stress, products, filtered, sums, 2 + t + (t // 2) * (own - 4), tiles
        ),
    )
    for n in range(2):
        value = sums[n]
        folded = value[:, : value.shape[1] // 2] + value[:, value.shape[1] // 2 :]
        totals[n : n + 1] = jnp.sum(folded.T, axis=0, keepdims=True)


def final_kernel(totals, strength_inner, strength_outer, coefficient, viscosity):
    own, rows = viscosity.shape[0], viscosity.shape[1]
    tall = totals.shape[1]
    wall_index, wall_count = lax.axis_index("gy"), lax.axis_size("gy")
    raw = jnp.clip(8.0 * totals[0:1] / totals[1:2], 0.0, clip_high)
    plane = lax.broadcasted_iota(jnp.int32, (rows, tall), 0)
    entry = lax.broadcasted_iota(jnp.int32, (rows, tall), 1)
    below = jnp.where(plane == 0, jnp.where(wall_index == 0, 0, rows + 1), plane - 1)
    last = plane == rows - 1
    above = jnp.where(last, jnp.where(wall_index == wall_count - 1, rows - 1, rows + 5), plane + 1)
    spread = jnp.broadcast_to(raw, (rows, tall))
    parts = [
        jnp.where(entry == pick, spread * weight, 0.0)
        for pick, weight in ((below, 0.25), (plane, 0.5), (above, 0.25))
    ]
    column = jnp.sum((parts[0] + parts[2]) + parts[1], axis=1, keepdims=True)
    square = jnp.where(plane[:, :rows] == entry[:, :rows], column, 0.0)
    coefficient[...] = jnp.sum(square, axis=0, keepdims=True)
    for i in range(own):
        source = strength_outer[i // (own - 1)] if i in (0, own - 1) else strength_inner[i - 1]
        viscosity[i] = column * source


def shift(count, step, closed):
    pairs = [(i, i + step) for i in range(count)]
    if closed:
        return [(i, j % count) for i, j in pairs]
    return [(i, j) for i, j in pairs if 0 <= j < count]


def vmem(n):
    return [pl.BlockSpec(memory_space=pltpu.VMEM)] * n


def anywhere(n):
    return [pl.BlockSpec(memory_space=pl.ANY)] * n


def sum_over(value, axis):
    count = lax.axis_size(axis)
    if count & (count - 1):
        return lax.psum(value, axis)
    step = 1
    while step < count:
        value = value + lax.ppermute(value, axis, [(i, i ^ step) for i in range(count)])
        step *= 2
    return value


def local(v):
    _, own, rows, span = v.shape
    wall_count = lax.axis_size("gy")
    stream_count = lax.axis_size("gx")
    float_array = functools.partial(jax.ShapeDtypeStruct, dtype=jnp.float32)

    to_next = shift(stream_count, 1, True)
    to_last = shift(stream_count, -1, True)
    sent_left = v[:, own - 2 :]
    later, sent_left = lax.optimization_barrier((v, sent_left))
    low = lax.ppermute(v[:, :, rows - 2 :], "gy", shift(wall_count, 1, False))
    high = lax.ppermute(v[:, :, :2], "gy", shift(wall_count, -1, False))
    left = lax.ppermute(sent_left, "gx", to_next)
    right = lax.ppermute(later[:, :2], "gx", to_last)
    edges = jnp.concatenate([low, high], axis=2)
    left_edge = lax.ppermute(edges[:, own - 2 :], "gx", to_next)
    right_edge = lax.ppermute(edges[:, :2], "gx", to_last)

    tall = rows + TILE
    wide = own + 4
    kept = tuple(
        float_array((fields, sum(count for _, count in spans), tall, span))
        for fields, spans in zip((6, 6, 3, 3), kept_rows(own))
    )
    fields = [pltpu.VMEM((n, wide, tall, span), jnp.float32) for n in (6, 6, 3, 3)]
    cells = pltpu.VMEM((3, wide, tall, span), jnp.float32)
    params = pltpu.CompilerParams(vmem_limit_bytes=30 * 1024 * 1024)
    inner = pl.pallas_call(
        inner_kernel,
        out_shape=(float_array((2, tall, span)), float_array((own - 2, rows, span))) + kept,
        in_specs=anywhere(1) + vmem(2),
        out_specs=tuple(vmem(2) + anywhere(4)),
        scratch_shapes=fields + [cells, pltpu.SemaphoreType.DMA((9,))],
        compiler_params=params,
        cost_estimate=pl.CostEstimate(flops=60_000_000, transcendentals=0, bytes_accessed=6_000_000),
        name="inner",
    )(v, low, high)
    sums, strength_inner = inner[:2]
    totals, strength_outer = pl.pallas_call(
        outer_kernel,
        out_shape=(float_array((2, tall)), float_array((2, rows, span))),
        in_specs=anywhere(3) + vmem(4) + anywhere(4) + vmem(1),
        out_specs=tuple(vmem(2)),
        scratch_shapes=fields
        + [pltpu.VMEM((2, tall, span), jnp.float32), cells, pltpu.SemaphoreType.DMA((12,))],
        compiler_params=params,
        cost_estimate=pl.CostEstimate(flops=40_000_000, transcendentals=0, bytes_accessed=6_000_000),
        name="outer",
    )(v, left, right, low, high, left_edge, right_edge, *inner[2:], sums)

    totals = sum_over(totals, "gx")
    coefficient, viscosity = pl.pallas_call(
        final_kernel,
        out_shape=(float_array((1, rows)), float_array((own, rows, span))),
        in_specs=vmem(3),
        out_specs=tuple(vmem(2)),
        compiler_params=pltpu.CompilerParams(vmem_limit_bytes=8 * 1024 * 1024),
        name="final",
    )(totals, strength_inner, strength_outer)
    return coefficient[0], viscosity


def solution(mesh):
    in_specs = (P(None, "gx", "gy", None),)
    out_specs = (P("gy"), P("gx", "gy", None))
    return jax.shard_map(local, mesh=mesh, in_specs=in_specs, out_specs=out_specs, check_vma=False)
```
